32 devices in a mesh: env: 32 (over z, y, x, core).
Axes of the slice: x: 2, y: 2, z: 4, core: 2. Of those that a mesh axis runs over, the one named last changes fastest.
Arguments:
- observations: bfloat16 [16, 512, 96], P(None, 'env'), may hold values from -6 to 6
- physics_params: bfloat16 [512, 32], P('env'), may hold values from -4 to 4
- actions: int32 [16, 512, 20], P(None, 'env'), may hold values from 0 to 10
- reset_step: int32 [512], P('env'), may hold values from 0 to 16
- hidden_start: bfloat16 [512, 1024], P('env'), may hold values from -0.8984375 to 0.8984375
- cell_start: float32 [512, 1024], P('env'), may hold values from -4 to 4
- old_logp: float32 [16, 512], P(None, 'env'), may hold values from -50.5 to -47.5
- advantages: float32 [16, 512], P(None, 'env'), may hold values from 3 to 7
- returns: float32 [16, 512], P(None, 'env'), may hold values from -5 to 5
- lstm_weight: bfloat16 [1152, 4096], replicated, may hold values from -0.1875 to 0.1875
- lstm_bias: float32 [4096], replicated, may hold values from -4 to 4
- head_weight: bfloat16 [1024, 221], replicated, may hold values from -0.1875 to 0.1875
Outputs:
- lstm_step: float32 [1152, 4096], P('env')
- bias_step: float32 [4096], P('env')
- head_step: float32 [1024, 221], P('env')
- kl_mean: float32 [], replicated
The draws below stay inside these ranges and needn't reach their ends.
All inputs are finite; a program needn't handle non-finite values.
Results may differ from the reference program's by a relative error of at most 0.0073.
Values sent between devices are 32-bit elements; how exact they have to be, the bound alone decides.
A program may use at most 128 MiB of HBM per device.

```python
import math
import jax
import jax.numpy as jnp
from jax import lax

H = 1024
OBS = 96
PHYS = 32
ACT = 20
BINS = 11
STEPS = 16
IN = 128
ENVS = 512


def with_ends(entries, key, least, largest):
    extent = entries.shape
    spot = [jax.random.randint(jax.random.fold_in(key, axis), (), 0, extent[axis]) for axis in range(len(extent))]
    entries = entries.at[tuple(spot)].set(least)
    longest = extent.index(max(extent))
    spot[longest] = (spot[longest] + 1) % extent[longest]
    return entries.at[tuple(spot)].set(largest)


def shard_levels(stream_key, shape, pieces, low, high):
    level, own = 1.0, jax.random.fold_in(stream_key, 6)
    for position, parts in pieces:
        heights = jnp.exp(jax.random.uniform(jax.random.fold_in(own, position), (parts,), jnp.float32, low / len(pieces), high / len(pieces)))
        level = level * jnp.repeat(heights, shape[position] // parts).reshape([-1 if axis == position else 1 for axis in range(len(shape))])
    return level


def gaussian(rng, shape, scale, reach, cuts=(), kind=jnp.bfloat16):
    gain = shard_levels(rng, shape, cuts, -0.22, 0.18) if cuts else 1.0
    entries = jax.random.normal(rng, shape, jnp.float32) * scale * gain
    return jnp.minimum(jnp.maximum(entries, -reach), reach).astype(kind)


def setup_inputs(seed: int = 0) -> dict:
    streams_of = jax.random.split(jax.random.key(seed), 13)
    observations = gaussian(streams_of[0], (STEPS, ENVS, OBS), 1.0, 6.0, ((1, 32),))
    physics_params = gaussian(streams_of[1], (ENVS, PHYS), 1.0, 4.0, ((0, 32),))
    actions = with_ends(jax.random.randint(streams_of[2], (STEPS, ENVS, ACT), 0, BINS), jax.random.fold_in(streams_of[2], 1), 0, BINS - 1).astype(jnp.int32)
    reset_step = with_ends(jax.random.randint(streams_of[3], (ENVS,), 0, STEPS + 1), jax.random.fold_in(streams_of[3], 1), 0, STEPS).astype(jnp.int32)
    hidden_start = jnp.clip(jax.random.uniform(streams_of[4], (ENVS, H), jnp.float32, -0.8984375, 0.8984375) * shard_levels(streams_of[4], (ENVS, H), ((0, 32),), -0.4, 0.0), -0.8984375, 0.8984375).astype(jnp.bfloat16)
    cell_start = gaussian(streams_of[5], (ENVS, H), 1.0, 4.0, ((0, 32),), jnp.float32)
    old_logp = jnp.clip(-50.5 + 3.0 * jax.random.uniform(streams_of[6], (STEPS, ENVS), jnp.float32) ** shard_levels(streams_of[6], (STEPS, ENVS), ((1, 32),), -0.2, 0.2), -50.5, -47.5)
    advantages = jnp.clip(3.0 + 4.0 * jax.random.uniform(streams_of[7], (STEPS, ENVS), jnp.float32) ** shard_levels(streams_of[7], (STEPS, ENVS), ((1, 32),), -0.2, 0.2), 3.0, 7.0)
    returns = gaussian(streams_of[8], (STEPS, ENVS), 1.0, 5.0, ((1, 32),), jnp.float32)
    lstm_weight = gaussian(streams_of[9], (IN + H, 4 * H), (IN + H) ** -0.5, 0.1875)
    lstm_bias = gaussian(streams_of[10], (4 * H,), 1.0, 4.0, (), jnp.float32)
    head_weight = gaussian(streams_of[11], (H, ACT * BINS + 1), H ** -0.5, 0.1875)
    return dict(observations=observations, physics_params=physics_params, actions=actions, reset_step=reset_step, hidden_start=hidden_start, cell_start=cell_start, old_logp=old_logp, advantages=advantages, returns=returns, lstm_weight=lstm_weight, lstm_bias=lstm_bias, head_weight=head_weight)


kl_coef = 0.5
value_coef = 0.5
spread_floor = 0.25

def local_terms(observations, physics_params, actions, reset_step, hidden_start, cell_start, old_logp, norm_adv, returns, lstm_weight, lstm_bias, head_weight):
    step_count, env_count = (observations.shape[0], observations.shape[1])
    hidden = hidden_start.shape[1]
    width_in = lstm_weight.shape[0] - hidden
    act_count = actions.shape[2]
    bin_count = (head_weight.shape[1] - 1) // act_count
    phys_tiled = jnp.broadcast_to(physics_params[None], (step_count, env_count, physics_params.shape[1]))
    inputs = jnp.concatenate([observations, phys_tiled], axis=2).reshape(step_count * env_count, width_in)
    w_rec = lstm_weight[width_in:]
    projected = jnp.dot(inputs, lstm_weight[:width_in], preferred_element_type=jnp.float32) + lstm_bias
    projected = projected.reshape(step_count, env_count, 4 * hidden)
    columns = lax.broadcasted_iota(jnp.int32, (1, 4 * hidden), 1)
    is_cand = (columns >= 2 * hidden) & (columns < 3 * hidden)
    step_ids = jnp.arange(step_count, dtype=jnp.int32)

    def advance(state_pair, inputs_now):
        h_prev, c_prev = state_pair
        proj_now, step_index = inputs_now
        keep_mask = (reset_step != step_index)[:, None]
        h_kept = jnp.where(keep_mask, h_prev, jnp.zeros_like(h_prev))
        c_kept = jnp.where(keep_mask, c_prev, jnp.zeros_like(c_prev))
        pre_act = proj_now + jnp.dot(h_kept, w_rec, preferred_element_type=jnp.float32)
        activated = jnp.where(is_cand, jnp.tanh(pre_act), jax.nn.sigmoid(pre_act))
        gate_i = activated[:, :hidden]
        gate_f = activated[:, hidden:2 * hidden]
        cand_gate = activated[:, 2 * hidden:3 * hidden]
        gate_o = activated[:, 3 * hidden:]
        c_new = gate_f * c_kept + gate_i * cand_gate
        tanh_c = jnp.tanh(c_new)
        h_new = (gate_o * tanh_c).astype(jnp.bfloat16)
        return ((h_new, c_new), (h_kept, c_kept, activated, tanh_c, h_new))
    final_state, saved = lax.scan(advance, (hidden_start, cell_start), (projected, step_ids))
    h_kept_all, c_kept_all, activated_all, tanh_all, hseq = saved
    h_flat = hseq.reshape(step_count * env_count, hidden)
    logits = jnp.dot(h_flat, head_weight, preferred_element_type=jnp.float32)
    policy = logits[:, :act_count * bin_count].reshape(-1, act_count, bin_count)
    value_pred = logits[:, act_count * bin_count]
    exp_policy = jnp.exp(policy)
    sum_exp = lax.optimization_barrier(jnp.sum(exp_policy, axis=2, keepdims=True))
    soft_probs = exp_policy / sum_exp
    log_probs = policy - jnp.log(sum_exp)
    levels = lax.broadcasted_iota(jnp.int32, (1, 1, bin_count), 2)
    onehot = (actions.reshape(-1, act_count)[:, :, None] == levels).astype(jnp.float32)
    token_logp = lax.optimization_barrier(jnp.sum(onehot * log_probs, axis=(1, 2)))
    log_ratio = token_logp - old_logp.reshape(-1)
    prob_ratio = jnp.exp(log_ratio)
    kl_part = jnp.sum(prob_ratio - 1.0 - log_ratio)
    grad_logp = kl_coef * (prob_ratio - 1.0) - norm_adv.reshape(-1) * prob_ratio
    grad_policy = grad_logp[:, None, None] * (onehot - soft_probs)
    grad_value = value_coef * (value_pred - returns.reshape(-1))
    grad_logits = jnp.concatenate([grad_policy.reshape(-1, act_count * bin_count), grad_value[:, None]], axis=1).astype(jnp.bfloat16)
    head_grad = lax.dot_general(h_flat, grad_logits, (((0,), (0,)), ((), ())), preferred_element_type=jnp.float32)
    from_head = lax.dot_general(grad_logits, head_weight, (((1,), (1,)), ((), ())), preferred_element_type=jnp.float32)
    from_head = from_head.reshape(step_count, env_count, hidden)

    def retreat(state_pair, inputs_now):
        grad_h_next, grad_c_next = state_pair
        c_kept, activated, tanh_c, head_part, step_index = inputs_now
        keep_mask = (reset_step != step_index)[:, None]
        gate_i = activated[:, :hidden]
        gate_f = activated[:, hidden:2 * hidden]
        cand_gate = activated[:, 2 * hidden:3 * hidden]
        gate_o = activated[:, 3 * hidden:]
        grad_h = head_part + grad_h_next
        grad_c = grad_c_next + grad_h * gate_o * (1.0 - tanh_c * tanh_c)
        upstream = jnp.concatenate([grad_c * cand_gate, grad_c * c_kept, grad_c * gate_i, grad_h * tanh_c], axis=1)
        act_slope = jnp.where(is_cand, 1.0 - activated * activated, activated * (1.0 - activated))
        grad_gates = (upstream * act_slope).astype(jnp.bfloat16)
        grad_h_prev = lax.dot_general(grad_gates, w_rec, (((1,), (1,)), ((), ())), preferred_element_type=jnp.float32)
        grad_h_prev = jnp.where(keep_mask, grad_h_prev, jnp.zeros_like(grad_h_prev))
        grad_c_prev = jnp.where(keep_mask, grad_c * gate_f, jnp.zeros_like(grad_c))
        return ((grad_h_prev, grad_c_prev), grad_gates)
    zero_state = jnp.zeros((env_count, hidden), jnp.float32)
    final_grads, grad_gates = lax.scan(retreat, (zero_state, zero_state), (c_kept_all, activated_all, tanh_all, from_head, step_ids), reverse=True)
    operand = jnp.concatenate([inputs, h_kept_all.reshape(step_count * env_count, hidden)], axis=1)
    return (operand, grad_gates.reshape(step_count * env_count, 4 * hidden), head_grad, kl_part)

def reference(observations, physics_params, actions, reset_step, hidden_start, cell_start, old_logp, advantages, returns, lstm_weight, lstm_bias, head_weight):
    token_total = advantages.size
    adv_mean = jnp.sum(advantages) / token_total
    spread = jnp.sum((advantages - adv_mean) * (advantages - adv_mean)) / token_total
    norm_adv = (advantages - adv_mean) / jnp.sqrt(spread + spread_floor)
    env_total = observations.shape[1]
    env_block = math.gcd(env_total, 1024)
    block_count = env_total // env_block

    def take_block(source, block_index, axis_dim):
        return lax.dynamic_slice_in_dim(source, block_index * env_block, env_block, axis_dim)

    def add_block(running, block_index):
        operand, grad_gates, head_grad, kl_part = local_terms(take_block(observations, block_index, 1), take_block(physics_params, block_index, 0), take_block(actions, block_index, 1), take_block(reset_step, block_index, 0), take_block(hidden_start, block_index, 0), take_block(cell_start, block_index, 0), take_block(old_logp, block_index, 1), take_block(norm_adv, block_index, 1), take_block(returns, block_index, 1), lstm_weight, lstm_bias, head_weight)
        lstm_grad = lax.dot_general(operand, grad_gates, (((0,), (0,)), ((), ())), preferred_element_type=jnp.float32)
        bias_grad = lax.optimization_barrier(jnp.sum(grad_gates.astype(jnp.float32), axis=0))
        return ((running[0] + lstm_grad, running[1] + bias_grad, running[2] + head_grad, running[3] + kl_part), None)
    initial = (jnp.zeros(lstm_weight.shape, jnp.float32), jnp.zeros(lstm_bias.shape, jnp.float32), jnp.zeros(head_weight.shape, jnp.float32), jnp.zeros((), jnp.float32))
    running, unused = lax.scan(add_block, initial, jnp.arange(block_count, dtype=jnp.int32))
    param_total = lstm_weight.size + lstm_bias.size + head_weight.size
    grad_sq = jnp.sum(running[0] * running[0]) + jnp.sum(running[1] * running[1]) + jnp.sum(running[2] * running[2])
    scale = 1.0 / jnp.sqrt(grad_sq / param_total + 1.0)
    return (running[0] * scale, running[1] * scale, running[2] * scale, running[3] / token_total)
```

```python
import functools
import math

import jax
import jax.numpy as jnp
from jax import lax
from jax.experimental import pallas as pl
from jax.experimental.pallas import tpu as pltpu
from jax.sharding import PartitionSpec as P

kl_coef = 0.5
value_coef = 0.5
spread_floor = 0.25
f32 = jnp.float32
bf16 = jnp.bfloat16
MESH = pl.DeviceIdType.MESH
NT = (((1,), (1,)), ((), ()))
TN = (((0,), (0,)), ((), ()))


def sigmoid(x):
    return 0.5 * jnp.tanh(0.5 * x) + 0.5


def kernel(
    sizes,
    x_ref,
    act_ref,
    reset_ref,
    h0_ref,
    c0_ref,
    aux_ref,
    w_ref,
    bias_ref,
    hw_ref,
    same_ref,
    spread_ref,
    level_ref,
    dw_ref,
    db_ref,
    dh_ref,
    kl_ref,
    gates,
    ck_all,
    tc_all,
    hseq,
    hk_b,
    h_now,
    c_now,
    gg_b,
    head_part,
    all_h,
    all_g,
    all_x,
    hs_sem,
    hr_sem,
    fs_sem,
    fr_sem,
    gs_sem,
    gr_sem,
    xs_sem,
    xr_sem,
):
    steps, envs, hidden, width_in, group, policy_cols = sizes
    chips = group // 2
    me = lax.axis_index("env")
    mine = lax.rem(me, group)
    base = me - mine
    core = lax.rem(mine, 2)
    chip = mine // 2
    partner = chip * 2 + (1 - core)
    part = 4 * hidden // group
    chunk = 256

    def other(k):
        return lax.rem(mine + k, group)

    def same_core(k):
        return lax.rem(chip + k, chips) * 2 + core

    barrier = pltpu.get_barrier_semaphore()
    for k in range(1, group):
        pl.semaphore_signal(barrier, inc=1, device_id=(base + other(k),), device_id_type=MESH)
    pl.semaphore_wait(barrier, group - 1)

    def x_copy(k):
        return pltpu.make_async_remote_copy(
            src_ref=x_ref,
            dst_ref=all_x.at[mine],
            send_sem=xs_sem.at[k - 1],
            recv_sem=xr_sem.at[k - 1],
            device_id=(base + other(k),),
            device_id_type=MESH,
        )

    def h_copy(k, rows):
        return pltpu.make_async_remote_copy(
            src_ref=all_h.at[mine, rows],
            dst_ref=all_h.at[mine, rows],
            send_sem=hs_sem.at[k - 1],
            recv_sem=hr_sem.at[k - 1],
            device_id=(base + same_core(k),),
            device_id_type=MESH,
        )

    def forward_copy(k):
        block = same_core(k)
        return pltpu.make_async_remote_copy(
            src_ref=all_h.at[block],
            dst_ref=all_h.at[block],
            send_sem=fs_sem.at[k],
            recv_sem=fr_sem.at[k],
            device_id=(base + partner,),
            device_id_type=MESH,
        )

    def g_copy(k, rows):
        target = other(k)
        cols = pl.ds(pl.multiple_of(target * part, part), part)
        return pltpu.make_async_remote_copy(
            src_ref=gates.at[rows, cols],
            dst_ref=all_g.at[mine, rows],
            send_sem=gs_sem.at[k - 1],
            recv_sem=gr_sem.at[k - 1],
            device_id=(base + target,),
            device_id_type=MESH,
        )

    def rows_of(step):
        return pl.ds(pl.multiple_of(step * envs, envs), envs)

    every = pl.ds(0, steps * envs)

    for k in range(1, group):
        x_copy(k).start()

    x_b = x_ref[...].astype(bf16)
    for n in range(0, 4 * hidden, 512):
        gates[:, n : n + 512] = (
            jnp.dot(x_b, w_ref[:width_in, n : n + 512], preferred_element_type=f32)
            + bias_ref[:, n : n + 512]
        )
    h_now[...] = h0_ref[...].astype(f32)
    c_now[...] = c0_ref[...]

    def advance(step, carry):
        rows = rows_of(step)

        @pl.when(step > 0)
        def _():
            for k in range(1, chips):
                h_copy(k, rows_of(step - 1)).start()

        keep = reset_ref[...] != step
        h_kept = jnp.where(keep, h_now[...], 0.0)
        all_h[mine, rows, :] = h_kept
        hk_b[...] = h_kept.astype(bf16)
        for n in range(0, hidden, chunk):
            pre = []
            for gate in range(4):
                cols = slice(gate * hidden + n, gate * hidden + n + chunk)
                pre.append(
                    gates[rows, cols]
                    + jnp.dot(hk_b[...], w_ref[width_in:, cols], preferred_element_type=f32)
                )
            gi, gf, gc, go = (sigmoid(pre[0]), sigmoid(pre[1]), jnp.tanh(pre[2]), sigmoid(pre[3]))
            c_kept = jnp.where(keep, c_now[:, n : n + chunk], 0.0)
            c_new = gf * c_kept + gi * gc
            tc = jnp.tanh(c_new)
            h_new = (go * tc).astype(bf16)
            for gate, value in enumerate((gi, gf, gc, go)):
                gates[rows, gate * hidden + n : gate * hidden + n + chunk] = value
            ck_all[rows, n : n + chunk] = c_kept
            tc_all[rows, n : n + chunk] = tc
            c_now[:, n : n + chunk] = c_new
            h_now[:, n : n + chunk] = h_new.astype(f32)
            hseq[rows, n : n + chunk] = h_new
        return carry

    lax.fori_loop(0, steps, advance, 0)
    for k in range(1, chips):
        h_copy(k, rows_of(steps - 1)).start()

    logits = jnp.dot(hseq[...], hw_ref[...], preferred_element_type=f32)
    col = lax.broadcasted_iota(jnp.int32, logits.shape, 1)
    is_policy = col < policy_cols
    policy = jnp.where(is_policy, logits, 0.0)
    exp_policy = jnp.where(is_policy, jnp.exp(policy), 0.0)
    sum_exp = jnp.dot(
        exp_policy, same_ref[...], preferred_element_type=f32, precision=lax.Precision.HIGHEST
    )
    sum_exp = jnp.where(is_policy, sum_exp, 1.0)
    probs = exp_policy / sum_exp
    log_probs = policy - jnp.log(sum_exp)
    taken = jnp.dot(act_ref[...], spread_ref[...], preferred_element_type=f32)
    hit = (taken == level_ref[...]) & is_policy
    token_logp = jnp.sum(jnp.where(hit, log_probs, 0.0), axis=1, keepdims=True)
    log_ratio = token_logp - aux_ref[:, 0:1]
    ratio = jnp.exp(log_ratio)
    kl_ref[...] = jnp.sum(ratio - 1.0 - log_ratio, axis=0, keepdims=True)
    grad_logp = kl_coef * (ratio - 1.0) - aux_ref[:, 1:2] * ratio
    grad_policy = grad_logp * (jnp.where(hit, 1.0, 0.0) - probs)
    grad_value = value_coef * (logits - aux_ref[:, 2:3])
    grad_logits = jnp.where(
        is_policy, grad_policy, jnp.where(col == policy_cols, grad_value, 0.0)
    ).astype(bf16)
    dh_ref[...] = lax.dot_general(hseq[...], grad_logits, TN, preferred_element_type=f32)
    head_part[...] = lax.dot_general(grad_logits, hw_ref[...], NT, preferred_element_type=f32)

    for k in range(1, chips):
        h_copy(k, every).wait_recv()
    for k in range(chips):
        forward_copy(k).start()

    h_now[...] = jnp.zeros_like(h_now)
    c_now[...] = jnp.zeros_like(c_now)

    def retreat(turn, carry):
        step = steps - 1 - turn
        rows = rows_of(step)

        @pl.when(turn > 0)
        def _():
            for k in range(1, group):
                g_copy(k, rows_of(step + 1)).start()

        keep = reset_ref[...] != step
        for n in range(0, hidden, chunk):
            here = slice(n, n + chunk)
            gi, gf, gc, go = (
                gates[rows, gate * hidden + n : gate * hidden + n + chunk] for gate in range(4)
            )
            tc = tc_all[rows, here]
            grad_h = head_part[rows, here] + h_now[:, here]
            grad_c = c_now[:, here] + grad_h * go * (1.0 - tc * tc)
            grads = (
                grad_c * gc * (gi * (1.0 - gi)),
                grad_c * ck_all[rows, here] * (gf * (1.0 - gf)),
                grad_c * gi * (1.0 - gc * gc),
                grad_h * tc * (go * (1.0 - go)),
            )
            for gate, value in enumerate(grads):
                rounded = value.astype(bf16)
                cols = slice(gate * hidden + n, gate * hidden + n + chunk)
                gg_b[:, cols] = rounded
                gates[rows, cols] = rounded.astype(f32)
            c_now[:, here] = jnp.where(keep, grad_c * gf, 0.0)
        for n in range(0, hidden, chunk):
            back = lax.dot_general(
                gg_b[...],
                w_ref[width_in + n : width_in + n + chunk, :],
                NT,
                preferred_element_type=f32,
            )
            h_now[:, n : n + chunk] = jnp.where(keep, back, 0.0)
        return carry

    lax.fori_loop(0, steps, retreat, 0)
    for k in range(1, group):
        g_copy(k, rows_of(0)).start()

    all_x[mine] = x_ref[...]
    all_g[mine] = gates[:, pl.ds(pl.multiple_of(mine * part, part), part)]
    db_ref[...] = jnp.sum(gates[...], axis=0, keepdims=True)

    for k in range(1, group):
        x_copy(k).wait()
    for k in range(1, chips):
        h_copy(k, every).wait_send()
    for k in range(chips):
        forward_copy(k).wait()
    for k in range(1, group):
        source = lax.rem(mine + k, group)
        cols = pl.ds(pl.multiple_of(source * part, part), part)
        g_copy(k, every).wait()

    dw_ref[...] = jnp.zeros_like(dw_ref)

    def gather(source, carry):
        g_b = all_g[source].astype(bf16)
        x_part = lax.dot_general(all_x[source].astype(bf16), g_b, TN, preferred_element_type=f32)
        dw_ref[:width_in, :] += x_part
        for n in range(0, hidden, chunk):
            h_b = all_h[source, :, n : n + chunk].astype(bf16)
            dw_ref[width_in + n : width_in + n + chunk, :] += lax.dot_general(
                h_b, g_b, TN, preferred_element_type=f32
            )
        return carry

    lax.fori_loop(0, group, gather, 0)


def shards(
    observations,
    physics_params,
    actions,
    reset_step,
    hidden_start,
    cell_start,
    old_logp,
    advantages,
    returns,
    lstm_weight,
    lstm_bias,
    head_weight,
):
    devices = lax.axis_size("env")
    group = math.gcd(devices, 8)
    slabs = devices // group
    steps, envs, obs = observations.shape
    hidden = hidden_start.shape[1]
    total_in, gate_cols = lstm_weight.shape
    width_in = total_in - hidden
    act_count = actions.shape[2]
    head_cols = head_weight.shape[1]
    policy_cols = head_cols - 1
    bins = policy_cols // act_count
    lanes = -(-head_cols // 128) * 128
    tokens = steps * envs
    token_total = tokens * devices
    part = gate_cols // group

    adv_sums = lax.psum(jnp.stack([jnp.sum(advantages), jnp.sum(advantages * advantages)]), "env")
    adv_mean = adv_sums[0] / token_total
    spread = adv_sums[1] / token_total - adv_mean * adv_mean
    norm_adv = (advantages - adv_mean) / jnp.sqrt(spread + spread_floor)
    aux = jnp.stack([old_logp.reshape(-1), norm_adv.reshape(-1), returns.reshape(-1)], axis=1)

    phys = jnp.broadcast_to(physics_params[None], (steps, envs, physics_params.shape[1]))
    x = jnp.concatenate([observations, phys], axis=2).reshape(tokens, width_in).astype(f32)
    act = jnp.pad(actions.reshape(tokens, act_count), ((0, 0), (0, 128 - act_count))).astype(bf16)
    head_wide = jnp.pad(head_weight, ((0, 0), (0, lanes - head_cols)))
    col = jnp.arange(lanes)
    joint = jnp.where(col < policy_cols, col // bins, -1)
    same = ((joint[:, None] == joint[None, :]) & (joint[:, None] >= 0)).astype(f32)
    spread_map = (jnp.arange(128)[:, None] == joint[None, :]).astype(bf16)
    level = (col % bins).astype(f32)[None, :]

    vmem = pl.BlockSpec(memory_space=pltpu.VMEM)
    dma = pltpu.SemaphoreType.DMA
    chips = group // 2
    dw, db, dh, kl = pl.pallas_call(
        functools.partial(kernel, (steps, envs, hidden, width_in, group, policy_cols)),
        out_shape=(
            jax.ShapeDtypeStruct((total_in, part), f32),
            jax.ShapeDtypeStruct((1, gate_cols), f32),
            jax.ShapeDtypeStruct((hidden, lanes), f32),
            jax.ShapeDtypeStruct((1, 1), f32),
        ),
        in_specs=[vmem] * 12,
        out_specs=(vmem,) * 4,
        scratch_shapes=[
            pltpu.VMEM((tokens, gate_cols), f32),
            pltpu.VMEM((tokens, hidden), f32),
            pltpu.VMEM((tokens, hidden), f32),
            pltpu.VMEM((tokens, hidden), bf16),
            pltpu.VMEM((envs, hidden), bf16),
            pltpu.VMEM((envs, hidden), f32),
            pltpu.VMEM((envs, hidden), f32),
            pltpu.VMEM((envs, gate_cols), bf16),
            pltpu.VMEM((tokens, hidden), f32),
            pltpu.VMEM((group, tokens, hidden), f32),
            pltpu.VMEM((group, tokens, part), f32),
            pltpu.VMEM((group, tokens, width_in), f32),
            dma((chips - 1,)),
            dma((chips - 1,)),
            dma((chips,)),
            dma((chips,)),
            dma((group - 1,)),
            dma((group - 1,)),
            dma((group - 1,)),
            dma((group - 1,)),
        ],
        compiler_params=pltpu.CompilerParams(
            collective_id=0, has_side_effects=True, vmem_limit_bytes=60 * 1024 * 1024
        ),
    )(
        x,
        act,
        reset_step[:, None],
        hidden_start,
        cell_start,
        aux,
        lstm_weight,
        lstm_bias[None, :],
        head_wide,
        same,
        spread_map,
        level,
    )

    small = jnp.concatenate(
        [dh[:, :head_cols].reshape(devices, -1), db.reshape(devices, -1)], axis=1
    )
    small_part = lax.psum_scatter(small, "env", scatter_dimension=0, tiled=True)[0]
    head_rows = hidden // devices
    head_part = small_part[: head_rows * head_cols].reshape(head_rows, head_cols)
    bias_part = small_part[head_rows * head_cols :]

    along = [[slab * group + j for slab in range(slabs)] for j in range(group)]
    inside = [[slab * group + j for j in range(group)] for slab in range(slabs)]
    slab_rows = total_in // slabs
    own_rows = total_in // devices
    dw = lax.psum_scatter(
        dw.reshape(slabs, slab_rows, part),
        "env",
        scatter_dimension=0,
        axis_index_groups=along,
        tiled=True,
    )
    dw = lax.all_to_all(
        dw.reshape(group, own_rows, part), "env", 0, 0, axis_index_groups=inside, tiled=True
    )
    lstm_part = dw.transpose(1, 0, 2).reshape(own_rows, gate_cols)
    local_squares = jnp.sum(dw * dw) + jnp.sum(small_part * small_part)
    totals = lax.psum(jnp.stack([local_squares, kl[0, 0]]), "env")
    param_total = lstm_weight.size + lstm_bias.size + head_weight.size
    scale = 1.0 / jnp.sqrt(totals[0] / param_total + 1.0)
    return (lstm_part * scale, bias_part * scale, head_part * scale, totals[1] / token_total)


def solution(mesh):
    in_specs = (
        P(None, "env", None),
        P("env", None),
        P(None, "env", None),
        P("env"),
        P("env", None),
        P("env", None),
        P(None, "env"),
        P(None, "env"),
        P(None, "env"),
        P(),
        P(),
        P(),
    )
    out_specs = (P("env", None), P("env"), P("env", None), P())
    return jax.shard_map(shards, mesh=mesh, in_specs=in_specs, out_specs=out_specs, check_vma=False)
```
